32 devices in a mesh: grp: 2 (over y), seq: 8 (over z, x), bat: 2 (over core).
Axes of the slice: x: 2, y: 2, z: 4, core: 2. Of those that a mesh axis runs over, the one named last changes fastest.
Arguments:
- queries: bfloat16 [16, 16, 192], P(('grp', 'bat')), parts along dimension 0, may hold values from -8 to 8
- latent_cache: bfloat16 [16, 4096, 576], P('grp', 'seq'), parts along dimension 0, may hold values from -128 to 128
- cache_lengths: int32 [16], P('grp'), parts along dimension 0, may hold values from 128 to 4096, as said below
- key_weight: bfloat16 [16, 128, 512], P('bat'), may hold values from -0.5 to 0.5
- value_weight: bfloat16 [16, 512, 128], P('bat'), may hold values from -0.25 to 0.25
Outputs:
- attended: bfloat16 [16, 16, 128], P(('grp', 'bat')), parts along dimension 0
The draws below stay inside these ranges and needn't reach their ends.
There are 2 independent parts, one for each index of `grp`. The reference program is written for one: setup_inputs(seed, part) draws one part's arguments, and reference() takes and returns one part's arrays. A program takes and returns all parts, laid end to end along the dimension named above; an argument that names none is the same for every part. Nothing has to cross between parts.
Inputs may be any that keep to these rules, and one draw needn't show every extreme that they name: `cache_lengths`: each entry is a multiple of 128; at least one request has all 4096 positions valid and at least one has fewer.
All inputs are finite; a program needn't handle non-finite values.
Results may differ from the reference program's by a relative error of at most 0.0085.
Values may be sent and summed in bfloat16 or wider, within the bound.
A program may use at most 64 MiB of HBM per device.

```python
import jax
import jax.numpy as jnp
from jax import lax

H = 16
DC = 512
DR = 64
DN = 128
DV = 128
REQ = 8
SEQ = 4096


def query_table(key):
    base_key = jax.random.fold_in(key, 101)
    values_all = 1.8 * jax.random.normal(base_key, (REQ, H, DN + DR), jnp.float32)
    return jnp.clip(values_all, -8.0, 8.0)


def draw_queries(key, part):
    return query_table(key).astype(jnp.bfloat16)


def draw_latent_cache(key, part):
    base_key = jax.random.fold_in(key, 202)
    values_all = jax.random.normal(base_key, (REQ, SEQ, DC + DR), jnp.float32)
    values_all = jnp.clip(values_all, -6.0, 6.0)
    return values_all.astype(jnp.bfloat16)


def draw_cache_lengths(key, part):
    blocks = SEQ // 128
    request_ids = jnp.arange(REQ, dtype=jnp.int32)
    blocks_used = jax.random.randint(jax.random.fold_in(key, 303), (REQ,), 1, blocks + 1)
    longest = jax.random.randint(jax.random.fold_in(key, 304), (), 0, REQ)
    offset = jax.random.randint(jax.random.fold_in(key, 305), (), 1, REQ)
    shortest = (longest + offset) % REQ
    short_blocks = jax.random.randint(jax.random.fold_in(key, 306), (), 1, blocks)
    blocks_used = jnp.where(request_ids == shortest, short_blocks, blocks_used)
    blocks_used = jnp.where(request_ids == longest, blocks, blocks_used)
    return (blocks_used * 128).astype(jnp.int32)


def block_levels(stream_key, shape, pieces, smallest, high):
    loudness, own = 1.0, jax.random.fold_in(stream_key, 6)
    for dim, shards_of in pieces:
        draws = jnp.exp(jax.random.uniform(jax.random.fold_in(own, dim), (shards_of,), jnp.float32, smallest / len(pieces), high / len(pieces)))
        loudness = loudness * jnp.repeat(draws, shape[dim] // shards_of).reshape([-1 if axis == dim else 1 for axis in range(len(shape))])
    return loudness


def gaussian(rng, dims, width, limit, pieces=(), kind=jnp.bfloat16):
    result = width * jax.random.normal(rng, dims, jnp.float32)
    if pieces:
        result = result * block_levels(rng, dims, pieces, -0.22, 0.18)
    return jnp.clip(result, -limit, limit).astype(kind)


def setup_inputs(seed: int = 0, part: int = 0) -> dict:
    seeds = jax.random.split(jax.random.key(seed), 6)
    part_splits = jax.random.split(jax.random.fold_in(seeds[5], part), 6)
    return {
        "queries": draw_queries(jax.random.fold_in(jax.random.fold_in(seeds[5], part), 71), part),
        "latent_cache": draw_latent_cache(jax.random.fold_in(jax.random.fold_in(seeds[5], part), 71), part),
        "cache_lengths": draw_cache_lengths(jax.random.fold_in(jax.random.fold_in(seeds[5], part), 71), part),
        "key_weight": gaussian(seeds[3], (H, DN, DC), DN ** -0.5, 0.5, ((0, 2),)),
        "value_weight": gaussian(seeds[4], (H, DC, DV), DC ** -0.5, 0.25, ((0, 2),)),
    }


def reference(queries, latent_cache, cache_lengths, key_weight, value_weight):
    scaling = (DN + DR) ** -0.5
    positions = jnp.arange(SEQ, dtype=jnp.int32)
    key_full = key_weight.astype(jnp.float32)
    value_full = value_weight.astype(jnp.float32)

    def single(inputs):
        query_row, cache_rows, length = inputs
        absorbed = jnp.einsum("hd,hdc->hc", query_row[:, :DN].astype(jnp.float32), key_full).astype(jnp.bfloat16)
        joined = jnp.concatenate([absorbed, query_row[:, DN:]], axis=1)
        scores = lax.dot_general(joined, cache_rows, (((1,), (1,)), ((), ())), preferred_element_type=jnp.float32) * scaling
        scores = jnp.where((positions < length)[None, :], scores, -jnp.inf)
        maxima = jnp.max(scores, axis=1, keepdims=True)
        weights = jnp.exp(scores - maxima)
        totals = jnp.sum(weights, axis=1, keepdims=True)
        latent_out = jnp.dot(weights.astype(jnp.bfloat16), cache_rows[:, :DC], preferred_element_type=jnp.float32) / totals
        projected = jnp.einsum("hc,hcd->hd", latent_out, value_full, precision=lax.Precision.HIGHEST)
        return projected.astype(jnp.bfloat16)

    return lax.map(single, (queries, latent_cache, cache_lengths))
```

```python
import functools

import jax
import jax.numpy as jnp
from jax import lax
from jax.experimental import pallas as pl
from jax.experimental.pallas import tpu as pltpu
from jax.sharding import PartitionSpec as P

MESH = pl.DeviceIdType.MESH
masked_score = -1e30
group = 8
pieces = 3
stat_rows = 8


def iota(shape, dim):
    return lax.broadcasted_iota(jnp.int32, shape, dim)


def split3(x):
    parts = []
    for _ in range(pieces):
        part = x.astype(jnp.bfloat16).astype(jnp.float32)
        parts.append(part)
        x = x - part
    return parts


def kernel(
    n_seq,
    lengths_far,
    queries,
    cache,
    key_weight,
    value_weight,
    out,
    lengths,
    own_q,
    other_q,
    columns,
    keys,
    values,
    flipped,
    got,
    sent,
    load_sems,
    column_sems,
    query_sems,
    send_sems,
    recv_sems,
    near_sem,
    all_sem,
):
    seq = lax.axis_index("seq")
    bat = lax.axis_index("bat")
    peer = 1 - bat
    half, _, width = queries.shape
    heads, nope, latent = key_weight.shape
    depth = value_weight.shape[2]
    shard = cache.shape[2]
    pairs = half * heads
    total_pairs = 2 * pairs
    copies = depth // pairs
    scaling = width ** (-0.5)

    load_q = pltpu.make_async_copy(queries, own_q, load_sems.at[0])
    load_k = pltpu.make_async_copy(key_weight, keys, load_sems.at[1])
    load_v = pltpu.make_async_copy(value_weight, values, load_sems.at[2])
    load_lengths = pltpu.make_async_copy(lengths_far, lengths, load_sems.at[3])
    load_columns = [
        pltpu.make_async_copy(
            cache.at[(bat if i < half else peer) * half + i % half], columns.at[i], column_sems.at[i]
        )
        for i in range(2 * half)
    ]
    def start_pieces(source, target, sem, parts):
        size = heads // parts
        for j in range(parts):
            piece = pl.ds(j * size, size)
            pltpu.make_async_copy(source.at[piece], target.at[piece], sem).start()

    load_q.start()
    load_lengths.start()
    start_pieces(key_weight, keys, load_sems.at[1], 8)
    for copy in load_columns:
        copy.start()
    start_pieces(value_weight, values, load_sems.at[2], 8)

    barrier = pltpu.get_barrier_semaphore()

    def greet(step, _):
        far = lax.rem(seq + step, n_seq)
        pl.semaphore_signal(
            barrier, inc=1, device_id={"seq": far, "bat": 1}, device_id_type=MESH
        )
        return 0

    @pl.when(bat == 1)
    def _():
        pl.semaphore_signal(barrier, inc=1, device_id={"bat": peer}, device_id_type=MESH)

    lax.fori_loop(1, n_seq, greet, 0)

    def joined_rows(q_ref):
        q = q_ref[...].astype(jnp.float32)
        mine = jnp.where(bat == 0, q[:, :heads], q[:, heads:]).reshape(pairs, width)
        plain = mine[:, :nope]
        head_of = iota((pairs, nope), 0) % heads
        spread = jnp.concatenate(
            [jnp.where(head_of == h, plain, 0.0) for h in range(heads)], axis=1
        ).astype(jnp.bfloat16)
        absorbed = jnp.dot(
            spread, keys[...].reshape(heads * nope, latent), preferred_element_type=jnp.float32
        )
        return jnp.concatenate([absorbed, mine[:, nope:]], axis=1)

    def score(joined, i):
        piece = joined[(i % half) * heads : (i % half + 1) * heads].astype(jnp.bfloat16)
        scores = lax.dot_general(
            piece, columns[i], (((1,), (0,)), ((), ())), preferred_element_type=jnp.float32
        )
        owner = bat if i < half else peer
        left = lengths[owner * half + i % half] - seq * shard
        return jnp.where(iota(scores.shape, 1) < left, scores * scaling, masked_score)

    def soften(scores):
        highest = jnp.max(scores, axis=1, keepdims=True)
        weights = jnp.exp(scores - highest)
        return highest, jnp.sum(weights, axis=1, keepdims=True), weights.astype(jnp.bfloat16)

    def flip(i):
        flipped[i] = columns[i, :latent].T

    def weigh(weights, i):
        return jnp.dot(weights, flipped[i], preferred_element_type=jnp.float32)

    def send(source, far, side, index):
        return pltpu.make_async_remote_copy(
            src_ref=source,
            dst_ref=got.at[bat, seq],
            send_sem=send_sems.at[index],
            recv_sem=recv_sems.at[bat],
            device_id={"seq": far, "bat": side},
            device_id_type=MESH,
        )

    @pl.when(bat == 0)
    def _():
        pl.semaphore_wait(barrier, 1)
        pl.semaphore_signal(near_sem, inc=1, device_id={"bat": peer}, device_id_type=MESH)

    @pl.when(bat == 1)
    def _():
        pl.semaphore_wait(near_sem, 1)

    swap = pltpu.make_async_remote_copy(
        src_ref=own_q,
        dst_ref=other_q,
        send_sem=query_sems.at[0],
        recv_sem=query_sems.at[1],
        device_id={"bat": peer},
        device_id_type=MESH,
    )
    load_q.wait()
    swap.start()
    load_lengths.wait()
    load_k.wait()
    joined = joined_rows(own_q)

    lane = iota((heads, depth), 1)
    slot = lax.rem(lane, pairs)
    row = iota((heads, depth), 0)
    maxima = [jnp.zeros((heads, depth), jnp.float32)] * 2
    totals = [jnp.zeros((heads, depth), jnp.float32)] * 2
    sums = []
    scores, softened = {}, {}
    steps = [(i, i + 1) for i in range(0, 2 * half, 2)]
    lag = 1
    for t in range(len(steps) + lag):
        if t < len(steps):
            if t == 1:
                swap.wait()
            for i in steps[t]:
                load_columns[i].wait()
            for i in steps[t]:
                scores[i] = score(joined if i < half else other, i)
            if t == 1:
                other = joined_rows(other_q)
            for i in steps[t]:
                flip(i)
        def softs():
            if 1 <= t <= len(steps):
                for i in steps[t - 1]:
                    highest, total, softened[i] = soften(scores[i])
                    side = i // half
                    here = slot == (i % half) * heads + row
                    maxima[side] = jnp.where(here, highest, maxima[side])
                    totals[side] = jnp.where(here, total, totals[side])
        if lag == 1:
            softs()
        if lag <= t:
            for i in steps[t - lag]:
                sums.append(weigh(softened[i], i))
        if lag == 2:
            softs()

    load_v.wait()
    sums = jnp.concatenate(sums, axis=0)
    head_of = iota((total_pairs, latent), 0) % heads
    spread = jnp.concatenate(
        [jnp.where(head_of == h, sums, 0.0).astype(jnp.bfloat16) for h in range(heads)], axis=1
    )
    result = jnp.dot(
        spread, values[...].reshape(heads * latent, depth), preferred_element_type=jnp.float32
    ).astype(jnp.bfloat16)
    stats = []
    sub = iota((stat_rows, depth), 0)
    for side in range(2):
        rows = split3(jnp.sum(maxima[side], axis=0, keepdims=True))
        rows += split3(jnp.sum(totals[side], axis=0, keepdims=True))
        tile = jnp.zeros((stat_rows, depth), jnp.float32)
        for j, line in enumerate(rows):
            tile = jnp.where(sub == j, line, tile)
        stats.append(tile.astype(jnp.bfloat16))
    got[bat, seq, :pairs] = result[:pairs]
    got[bat, seq, pairs:] = stats[0]
    sent[:pairs] = result[pairs:]
    sent[pairs:] = stats[1]

    @pl.when(bat == 1)
    def _():
        pl.semaphore_wait(barrier, 2 * (n_seq - 1))
        pl.semaphore_signal(all_sem, inc=1, device_id={"bat": peer}, device_id_type=MESH)

    @pl.when(bat == 0)
    def _():
        pl.semaphore_wait(all_sem, 1)

    def send_all(step, _):
        far = jnp.where(2 * seq < n_seq, n_seq - 1 - step, step)
        send(sent, far, peer, 1).start()

        @pl.when(far != seq)
        def _():
            send(got.at[bat, seq], far, bat, 0).start()

        return 0

    lax.fori_loop(0, n_seq, send_all, 0)

    def settle(ref, sem):
        pltpu.make_async_copy(ref, ref, sem).wait()

    few = pl.ds(0, n_seq - 1)
    settle(got.at[0, few], recv_sems.at[bat])
    settle(got.at[0], recv_sems.at[peer])

    lane = iota((group, depth), 1)
    sub = iota((group, depth), 0)
    picked = iota((pairs, depth), 0) == iota((pairs, depth), 1) % pairs
    for side in range(2):
        peaks, sizes = [], []
        for start in range(0, n_seq, group):
            peak = jnp.zeros((group, depth), jnp.float32)
            size = jnp.zeros((group, depth), jnp.float32)
            for j in range(group):
                tile = got[side, start + j, pairs:].astype(jnp.float32)
                top = jnp.sum(jnp.where(sub < pieces, tile, 0.0), axis=0, keepdims=True)
                sum_ = jnp.sum(jnp.where(sub < pieces, 0.0, tile), axis=0, keepdims=True)
                peak = jnp.where(sub == j, top, peak)
                size = jnp.where(sub == j, sum_, size)
            peaks.append(peak)
            sizes.append(size)
        top = functools.reduce(jnp.maximum, peaks)
        top = jnp.max(top, axis=0, keepdims=True)
        factors = [jnp.exp(peak - top) for peak in peaks]
        whole = functools.reduce(jnp.add, [f * s for f, s in zip(factors, sizes)])
        whole = jnp.sum(whole, axis=0, keepdims=True)
        spread = []
        for factor in factors:
            scaled = factor / whole
            for start in range(0, group, copies):
                line = jnp.sum(
                    jnp.where(sub == start + lane // pairs, scaled, 0.0), axis=0, keepdims=True
                )
                spread.append(jnp.where(picked, line, 0.0))
        spread = jnp.concatenate(spread, axis=1)
        high = spread.astype(jnp.bfloat16)
        low = (spread - high.astype(jnp.float32)).astype(jnp.bfloat16)
        merged = jnp.dot(
            jnp.concatenate([high, low], axis=0),
            got[side, :, :pairs].reshape(n_seq * pairs, depth),
            preferred_element_type=jnp.float32,
        )
        merged = (merged[:pairs] + merged[pairs:]).reshape(half, heads, depth)
        out[:, side * heads : (side + 1) * heads, :] = merged.astype(jnp.bfloat16)

    settle(got.at[0], send_sems.at[1])
    settle(got.at[0, few], send_sems.at[0])


def per_device(n_seq, queries, latent_cache, cache_lengths, key_weight, value_weight):
    half, all_heads, _ = queries.shape
    heads = key_weight.shape[0]
    depth = value_weight.shape[2]
    pairs = half * heads
    latent = key_weight.shape[2]
    shard = latent_cache.shape[1]
    columns = jnp.swapaxes(latent_cache, 1, 2)
    vmem, anywhere = pltpu.VMEM, pl.BlockSpec(memory_space=pltpu.HBM)
    dma = pltpu.SemaphoreType.DMA
    operands = (cache_lengths, queries, columns, key_weight, value_weight)
    held = [pltpu.with_memory_space_constraint(x, pltpu.HBM) for x in operands]
    return pl.pallas_call(
        functools.partial(kernel, n_seq),
        out_shape=jax.ShapeDtypeStruct((half, all_heads, depth), jnp.bfloat16),
        in_specs=[anywhere] * 5,
        out_specs=pl.BlockSpec(memory_space=pltpu.VMEM),
        scratch_shapes=[
            pltpu.SMEM(cache_lengths.shape, cache_lengths.dtype),
            vmem(queries.shape, queries.dtype),
            vmem(queries.shape, queries.dtype),
            vmem(columns.shape, columns.dtype),
            vmem(key_weight.shape, key_weight.dtype),
            vmem(value_weight.shape, value_weight.dtype),
            vmem((8, shard, latent), jnp.bfloat16),
            vmem((2, n_seq, pairs + stat_rows, depth), jnp.bfloat16),
            vmem((pairs + stat_rows, depth), jnp.bfloat16),
            dma((4,)),
            dma((2 * half,)),
            dma((2,)),
            dma((2,)),
            dma((2,)),
            pltpu.SemaphoreType.REGULAR,
            pltpu.SemaphoreType.REGULAR,
        ],
        compiler_params=pltpu.CompilerParams(
            collective_id=0, has_side_effects=True, vmem_limit_bytes=32 << 20
        ),
    )(*held)


def solution(mesh):
    placed = (
        P(("grp", "bat"), None, None),
        P("grp", "seq", None),
        P("grp"),
        P("bat", None, None),
        P("bat", None, None),
    )
    return jax.shard_map(
        functools.partial(per_device, mesh.shape["seq"]),
        mesh=mesh,
        in_specs=placed,
        out_specs=P(("grp", "bat"), None, None),
        check_vma=False,
    )
```

```python
import functools

import jax
import jax.numpy as jnp
from jax import lax
from jax.experimental import pallas as pl
from jax.experimental.pallas import tpu as pltpu
from jax.sharding import PartitionSpec as P

MESH = pl.DeviceIdType.MESH
masked_score = -1e30
group = 8
pieces = 3
stat_rows = 8


def iota(shape, dim):
    return lax.broadcasted_iota(jnp.int32, shape, dim)


def split3(x):
    parts = []
    for _ in range(pieces):
        part = x.astype(jnp.bfloat16).astype(jnp.float32)
        parts.append(part)
        x = x - part
    return parts


def kernel(
    n_seq,
    lengths_far,
    queries,
    cache,
    key_weight,
    value_weight,
    out,
    lengths,
    own_q,
    other_q,
    columns,
    keys,
    values,
    flipped,
    got,
    sent,
    load_sems,
    column_sems,
    query_sems,
    send_sems,
    recv_sems,
    near_sem,
    all_sem,
):
    seq = lax.axis_index("seq")
    bat = lax.axis_index("bat")
    peer = 1 - bat
    half, _, width = queries.shape
    heads, nope, latent = key_weight.shape
    depth = value_weight.shape[2]
    shard = cache.shape[2]
    pairs = half * heads
    copies = depth // pairs
    scaling = width ** (-0.5)

    load_q = pltpu.make_async_copy(queries, own_q, load_sems.at[0])
    load_k = pltpu.make_async_copy(key_weight, keys, load_sems.at[1])
    load_v = pltpu.make_async_copy(value_weight, values, load_sems.at[2])
    load_lengths = pltpu.make_async_copy(lengths_far, lengths, load_sems.at[3])
    load_columns = [
        pltpu.make_async_copy(
            cache.at[(bat if i < half else peer) * half + i % half], columns.at[i], column_sems.at[i]
        )
        for i in range(2 * half)
    ]
    def start_pieces(source, target, sem, parts):
        size = heads // parts
        for j in range(parts):
            piece = pl.ds(j * size, size)
            pltpu.make_async_copy(source.at[piece], target.at[piece], sem).start()

    load_q.start()
    load_lengths.start()
    start_pieces(key_weight, keys, load_sems.at[1], heads)
    for copy in load_columns[:half]:
        copy.start()
    start_pieces(value_weight, values, load_sems.at[2], heads)
    for copy in load_columns[half:]:
        copy.start()

    barrier = pltpu.get_barrier_semaphore()

    def greet(step, _):
        far = lax.rem(seq + step, n_seq)
        pl.semaphore_signal(
            barrier, inc=1, device_id={"seq": far, "bat": 1}, device_id_type=MESH
        )
        return 0

    @pl.when(bat == 1)
    def _():
        pl.semaphore_signal(barrier, inc=1, device_id={"bat": peer}, device_id_type=MESH)

    lax.fori_loop(1, n_seq, greet, 0)

    def joined_rows(q_ref):
        q = q_ref[...].astype(jnp.float32)
        mine = jnp.where(bat == 0, q[:, :heads], q[:, heads:]).reshape(pairs, width)
        plain = mine[:, :nope]
        head_of = iota((pairs, nope), 0) % heads
        spread = jnp.concatenate(
            [jnp.where(head_of == h, plain, 0.0) for h in range(heads)], axis=1
        ).astype(jnp.bfloat16)
        absorbed = jnp.dot(
            spread, keys[...].reshape(heads * nope, latent), preferred_element_type=jnp.float32
        )
        return jnp.concatenate([absorbed, mine[:, nope:]], axis=1)

    def score(joined, i):
        piece = joined[(i % half) * heads : (i % half + 1) * heads].astype(jnp.bfloat16)
        scores = lax.dot_general(
            piece, columns[i], (((1,), (0,)), ((), ())), preferred_element_type=jnp.float32
        )
        owner = bat if i < half else peer
        left = lengths[owner * half + i % half] - seq * shard
        return jnp.where(iota(scores.shape, 1) < left, scores * scaling, masked_score)

    def soften(scores):
        highest = jnp.max(scores, axis=1, keepdims=True)
        weights = jnp.exp(scores - highest)
        return highest, jnp.sum(weights, axis=1, keepdims=True), weights

    def flip(i):
        flipped[i] = columns[i, :latent].T

    def weigh(weights, i):
        blank = jnp.zeros((heads, shard), jnp.float32)
        rows = [weights if k == i % half else blank for k in range(half)]
        return jnp.dot(
            jnp.concatenate(rows, axis=0).astype(jnp.bfloat16),
            flipped[i],
            preferred_element_type=jnp.float32,
        )

    def send(source, far, side, index):
        return pltpu.make_async_remote_copy(
            src_ref=source,
            dst_ref=got.at[bat, seq],
            send_sem=send_sems.at[index],
            recv_sem=recv_sems.at[bat],
            device_id={"seq": far, "bat": side},
            device_id_type=MESH,
        )

    @pl.when(bat == 0)
    def _():
        pl.semaphore_wait(barrier, 1)
        pl.semaphore_signal(near_sem, inc=1, device_id={"bat": peer}, device_id_type=MESH)

    @pl.when(bat == 1)
    def _():
        pl.semaphore_wait(near_sem, 1)

    swap = pltpu.make_async_remote_copy(
        src_ref=own_q,
        dst_ref=other_q,
        send_sem=query_sems.at[0],
        recv_sem=query_sems.at[1],
        device_id={"bat": peer},
        device_id_type=MESH,
    )
    load_q.wait()
    swap.start()
    load_lengths.wait()
    load_k.wait()
    joined = joined_rows(own_q)

    def project(side):
        stack = sums[side]
        head_of = iota((pairs, latent), 0) % heads
        spread = jnp.concatenate(
            [jnp.where(head_of == h, stack, 0.0).astype(jnp.bfloat16) for h in range(heads)], axis=1
        )
        result = jnp.dot(
            spread, values[...].reshape(heads * latent, depth), preferred_element_type=jnp.float32
        )
        sub = iota((stat_rows, depth), 0)
        rows = split3(jnp.sum(maxima[side], axis=0, keepdims=True))
        rows += split3(jnp.sum(totals[side], axis=0, keepdims=True))
        tile = jnp.zeros((stat_rows, depth), jnp.float32)
        for j, line in enumerate(rows):
            tile = jnp.where(sub == j, line, tile)
        return result.astype(jnp.bfloat16), tile.astype(jnp.bfloat16)

    def far_of(step):
        return jnp.where(2 * seq < n_seq, n_seq - 1 - step, step)

    def send_own(step, _):
        far = far_of(step)

        @pl.when(far != seq)
        def _():
            send(got.at[bat, seq], far, bat, 0).start()

        return 0

    def send_peer(step, _):
        send(sent, far_of(step), peer, 1).start()
        return 0

    lane = iota((heads, depth), 1)
    slot = lax.rem(lane, pairs)
    row = iota((heads, depth), 0)
    maxima = [jnp.zeros((heads, depth), jnp.float32)] * 2
    totals = [jnp.zeros((heads, depth), jnp.float32)] * 2
    sums, scores = [None, None], {}

    def arrive(items):
        for i in items:
            load_columns[i].wait()

    def score_all(items, joined):
        for i in items:
            scores[i] = score(joined, i)

    def flip_all(items):
        for i in items:
            flip(i)

    def weigh_all(items):
        weights = {}
        for i in items:
            side = i // half
            highest, total, weights[i] = soften(scores[i])
            here = slot == (i % half) * heads + row
            maxima[side] = jnp.where(here, highest, maxima[side])
            totals[side] = jnp.where(here, total, totals[side])
        for i in items:
            side = i // half
            part = weigh(weights[i], i)
            sums[side] = part if sums[side] is None else sums[side] + part

    first, second = range(half // 2), range(half // 2, half)
    lead, rest = (half,), range(half + 1, 2 * half)

    arrive(first)
    score_all(first, joined)
    flip_all(first)

    swap.wait()
    arrive(second)
    score_all(second, joined)
    other = joined_rows(other_q)
    flip_all(second)
    weigh_all(first)

    load_v.wait()
    arrive(lead)
    weigh_all(second)
    score_all(lead, other)
    result, tile = project(0)
    got[bat, seq, :pairs] = result
    got[bat, seq, pairs:] = tile
    flip_all(lead)

    @pl.when(bat == 1)
    def _():
        pl.semaphore_wait(barrier, 2 * (n_seq - 1))
        pl.semaphore_signal(all_sem, inc=1, device_id={"bat": peer}, device_id_type=MESH)

    @pl.when(bat == 0)
    def _():
        pl.semaphore_wait(all_sem, 1)

    early = n_seq // 4
    lax.fori_loop(0, early, send_own, 0)

    arrive(rest)
    score_all(rest, other)
    flip_all(rest)
    weigh_all((*lead, *rest))
    result, tile = project(1)
    sent[:pairs] = result
    sent[pairs:] = tile
    lax.fori_loop(0, early, send_peer, 0)

    def send_both(step, _):
        send_peer(step, 0)
        return send_own(step, 0)

    lax.fori_loop(early, n_seq, send_both, 0)

    def settle(ref, sem):
        pltpu.make_async_copy(ref, ref, sem).wait()

    few = pl.ds(0, n_seq - 1)
    settle(got.at[0, few], recv_sems.at[bat])
    settle(got.at[0], recv_sems.at[peer])

    lane = iota((group, depth), 1)
    sub = iota((group, depth), 0)
    picked = iota((pairs, depth), 0) == iota((pairs, depth), 1) % pairs
    for side in range(2):
        peaks, sizes = [], []
        for start in range(0, n_seq, group):
            peak = jnp.zeros((group, depth), jnp.float32)
            size = jnp.zeros((group, depth), jnp.float32)
            for j in range(group):
                tile = got[side, start + j, pairs:].astype(jnp.float32)
                top = jnp.sum(jnp.where(sub < pieces, tile, 0.0), axis=0, keepdims=True)
                sum_ = jnp.sum(jnp.where(sub < pieces, 0.0, tile), axis=0, keepdims=True)
                peak = jnp.where(sub == j, top, peak)
                size = jnp.where(sub == j, sum_, size)
            peaks.append(peak)
            sizes.append(size)
        top = functools.reduce(jnp.maximum, peaks)
        top = jnp.max(top, axis=0, keepdims=True)
        factors = [jnp.exp(peak - top) for peak in peaks]
        whole = functools.reduce(jnp.add, [f * s for f, s in zip(factors, sizes)])
        whole = jnp.sum(whole, axis=0, keepdims=True)
        spread = []
        for factor in factors:
            scaled = factor / whole
            for start in range(0, group, copies):
                line = jnp.sum(
                    jnp.where(sub == start + lane // pairs, scaled, 0.0), axis=0, keepdims=True
                )
                spread.append(jnp.where(picked, line, 0.0))
        spread = jnp.concatenate(spread, axis=1)
        high = spread.astype(jnp.bfloat16)
        low = (spread - high.astype(jnp.float32)).astype(jnp.bfloat16)
        merged = jnp.dot(
            jnp.concatenate([high, low], axis=0),
            got[side, :, :pairs].reshape(n_seq * pairs, depth),
            preferred_element_type=jnp.float32,
        )
        merged = (merged[:pairs] + merged[pairs:]).reshape(half, heads, depth)
        out[:, side * heads : (side + 1) * heads, :] = merged.astype(jnp.bfloat16)

    settle(got.at[0], send_sems.at[1])
    settle(got.at[0, few], send_sems.at[0])


def per_device(n_seq, queries, latent_cache, cache_lengths, key_weight, value_weight):
    half, all_heads, _ = queries.shape
    heads = key_weight.shape[0]
    depth = value_weight.shape[2]
    pairs = half * heads
    latent = key_weight.shape[2]
    shard = latent_cache.shape[1]
    columns = jnp.swapaxes(latent_cache, 1, 2)
    vmem, anywhere = pltpu.VMEM, pl.BlockSpec(memory_space=pltpu.HBM)
    dma = pltpu.SemaphoreType.DMA
    operands = (cache_lengths, queries, columns, key_weight, value_weight)
    held = [pltpu.with_memory_space_constraint(x, pltpu.HBM) for x in operands]
    return pl.pallas_call(
        functools.partial(kernel, n_seq),
        out_shape=jax.ShapeDtypeStruct((half, all_heads, depth), jnp.bfloat16),
        in_specs=[anywhere] * 5,
        out_specs=pl.BlockSpec(memory_space=pltpu.VMEM),
        scratch_shapes=[
            pltpu.SMEM(cache_lengths.shape, cache_lengths.dtype),
            vmem(queries.shape, queries.dtype),
            vmem(queries.shape, queries.dtype),
            vmem(columns.shape, columns.dtype),
            vmem(key_weight.shape, key_weight.dtype),
            vmem(value_weight.shape, value_weight.dtype),
            vmem((2 * half, shard, latent), columns.dtype),
            vmem((2, n_seq, pairs + stat_rows, depth), jnp.bfloat16),
            vmem((pairs + stat_rows, depth), jnp.bfloat16),
            dma((4,)),
            dma((2 * half,)),
            dma((2,)),
            dma((2,)),
            dma((2,)),
            pltpu.SemaphoreType.REGULAR,
            pltpu.SemaphoreType.REGULAR,
        ],
        compiler_params=pltpu.CompilerParams(
            collective_id=0, has_side_effects=True, vmem_limit_bytes=32 << 20
        ),
    )(*held)


def solution(mesh):
    placed = (
        P(("grp", "bat"), None, None),
        P("grp", "seq", None),
        P("grp"),
        P("bat", None, None),
        P("bat", None, None),
    )
    return jax.shard_map(
        functools.partial(per_device, mesh.shape["seq"]),
        mesh=mesh,
        in_specs=placed,
        out_specs=P(("grp", "bat"), None, None),
        check_vma=False,
    )
```

```python
import functools

import jax
import jax.numpy as jnp
from jax import lax
from jax.experimental import pallas as pl
from jax.experimental.pallas import tpu as pltpu
from jax.sharding import PartitionSpec as P

MESH = pl.DeviceIdType.MESH
masked_score = -1e30
group = 8
pieces = 3
stat_rows = 2 * pieces


def iota(shape, dim):
    return lax.broadcasted_iota(jnp.int32, shape, dim)


def split3(x):
    parts = []
    for _ in range(pieces):
        part = x.astype(jnp.bfloat16).astype(jnp.float32)
        parts.append(part)
        x = x - part
    return parts


def kernel(
    n_seq,
    lengths_far,
    queries,
    cache,
    key_weight,
    value_weight,
    out,
    lengths,
    own_q,
    other_q,
    columns,
    keys,
    values,
    flipped,
    got,
    sent,
    load_sems,
    column_sems,
    query_sems,
    send_sems,
    recv_sems,
    near_sem,
    all_sem,
):
    seq = lax.axis_index("seq")
    bat = lax.axis_index("bat")
    peer = 1 - bat
    half, _, width = queries.shape
    heads, nope, latent = key_weight.shape
    depth = value_weight.shape[2]
    shard = cache.shape[2]
    pairs = half * heads
    copies = depth // pairs
    scaling = width ** (-0.5)

    load_q = pltpu.make_async_copy(queries, own_q, load_sems.at[0])
    load_k = pltpu.make_async_copy(key_weight, keys, load_sems.at[1])
    load_v = pltpu.make_async_copy(value_weight, values, load_sems.at[2])
    load_lengths = pltpu.make_async_copy(lengths_far, lengths, load_sems.at[3])
    load_columns = [
        pltpu.make_async_copy(
            cache.at[(bat if i < half else peer) * half + i % half], columns.at[i], column_sems.at[i]
        )
        for i in range(2 * half)
    ]

    def start_pieces(source, target, sem, parts):
        size = heads // parts
        for j in range(parts):
            piece = pl.ds(j * size, size)
            pltpu.make_async_copy(source.at[piece], target.at[piece], sem).start()

    load_q.start()
    start_pieces(key_weight, keys, load_sems.at[1], heads)
    for copy in load_columns[:half]:
        copy.start()
    start_pieces(value_weight, values, load_sems.at[2], heads)
    for copy in load_columns[half:]:
        copy.start()
    load_lengths.start()

    barrier = pltpu.get_barrier_semaphore()

    def greet(step, _):
        far = lax.rem(seq + step, n_seq)
        pl.semaphore_signal(
            barrier, inc=1, device_id={"seq": far, "bat": 1}, device_id_type=MESH
        )
        return 0

    @pl.when(bat == 1)
    def _():
        pl.semaphore_signal(barrier, inc=1, device_id={"bat": peer}, device_id_type=MESH)

    lax.fori_loop(1, n_seq, greet, 0)

    def joined_rows(q_ref):
        q = q_ref[...].astype(jnp.float32)
        mine = jnp.where(bat == 0, q[:, :heads], q[:, heads:]).reshape(pairs, width)
        plain = mine[:, :nope]
        head_of = iota((pairs, nope), 0) % heads
        spread = jnp.concatenate(
            [jnp.where(head_of == h, plain, 0.0) for h in range(heads)], axis=1
        ).astype(jnp.bfloat16)
        absorbed = jnp.dot(
            spread, keys[...].reshape(heads * nope, latent), preferred_element_type=jnp.float32
        )
        return jnp.concatenate([absorbed, mine[:, nope:]], axis=1)

    def score(joined, i):
        piece = joined[(i % half) * heads : (i % half + 1) * heads].astype(jnp.bfloat16)
        scores = lax.dot_general(
            piece, columns[i], (((1,), (0,)), ((), ())), preferred_element_type=jnp.float32
        )
        owner = bat if i < half else peer
        left = lengths[owner * half + i % half] - seq * shard
        return jnp.where(iota(scores.shape, 1) < left, scores * scaling, masked_score)

    def soften(scores):
        highest = jnp.max(scores, axis=1, keepdims=True)
        weights = jnp.exp(scores - highest)
        return highest, jnp.sum(weights, axis=1, keepdims=True), weights

    def flip(i):
        flipped[i] = columns[i, :latent].T

    def weigh(weights, i):
        blank = jnp.zeros((heads, shard), jnp.float32)
        rows = [weights if k == i % half else blank for k in range(half)]
        return jnp.dot(
            jnp.concatenate(rows, axis=0).astype(jnp.bfloat16),
            flipped[i],
            preferred_element_type=jnp.float32,
        )

    def send(source, far, side, index):
        return pltpu.make_async_remote_copy(
            src_ref=source,
            dst_ref=got.at[bat, seq],
            send_sem=send_sems.at[index],
            recv_sem=recv_sems.at[bat],
            device_id={"seq": far, "bat": side},
            device_id_type=MESH,
        )

    @pl.when(bat == 0)
    def _():
        pl.semaphore_wait(barrier, 1)
        pl.semaphore_signal(near_sem, inc=1, device_id={"bat": peer}, device_id_type=MESH)

    @pl.when(bat == 1)
    def _():
        pl.semaphore_wait(near_sem, 1)

    swap = pltpu.make_async_remote_copy(
        src_ref=own_q,
        dst_ref=other_q,
        send_sem=query_sems.at[0],
        recv_sem=query_sems.at[1],
        device_id={"bat": peer},
        device_id_type=MESH,
    )
    load_q.wait()
    swap.start()
    load_lengths.wait()
    load_k.wait()
    joined = joined_rows(own_q)

    def project(side):
        stack = sums[side]
        head_of = iota((pairs, latent), 0) % heads
        spread = jnp.concatenate(
            [jnp.where(head_of == h, stack, 0.0).astype(jnp.bfloat16) for h in range(heads)], axis=1
        )
        result = jnp.dot(
            spread, values[...].reshape(heads * latent, depth), preferred_element_type=jnp.float32
        )
        sub = iota((stat_rows, depth), 0)
        rows = split3(jnp.sum(maxima[side], axis=0, keepdims=True))
        rows += split3(jnp.sum(totals[side], axis=0, keepdims=True))
        tile = jnp.zeros((stat_rows, depth), jnp.float32)
        for j, line in enumerate(rows):
            tile = jnp.where(sub == j, line, tile)
        return result.astype(jnp.bfloat16), tile.astype(jnp.bfloat16)

    def far_of(step):
        return jnp.where(2 * seq < n_seq, n_seq - 1 - step, step)

    def send_own(step, _):
        far = far_of(step)

        @pl.when(far != seq)
        def _():
            send(got.at[bat, seq], far, bat, 0).start()

        return 0

    def send_peer(step, _):
        send(sent, far_of(step), peer, 1).start()
        return 0

    lane = iota((heads, depth), 1)
    slot = lax.rem(lane, pairs)
    row = iota((heads, depth), 0)
    maxima = [jnp.zeros((heads, depth), jnp.float32)] * 2
    totals = [jnp.zeros((heads, depth), jnp.float32)] * 2
    sums, scores = [None, None], {}

    def arrive(items):
        for i in items:
            load_columns[i].wait()

    def score_all(items, joined):
        for i in items:
            scores[i] = score(joined, i)

    def flip_all(items):
        for i in items:
            flip(i)

    def weigh_all(items):
        weights = {}
        for i in items:
            side = i // half
            highest, total, weights[i] = soften(scores[i])
            here = slot == (i % half) * heads + row
            maxima[side] = jnp.where(here, highest, maxima[side])
            totals[side] = jnp.where(here, total, totals[side])
        for i in items:
            side = i // half
            part = weigh(weights[i], i)
            sums[side] = part if sums[side] is None else sums[side] + part

    first, second = range(half // 2), range(half // 2, half)
    lead, rest = (half,), range(half + 1, 2 * half)

    arrive(first)
    score_all(first, joined)
    flip_all(first)

    swap.wait()
    arrive(second)
    score_all(second, joined)
    other = joined_rows(other_q)
    flip_all(second)
    weigh_all(first)

    load_v.wait()
    arrive(lead)
    weigh_all(second)
    score_all(lead, other)
    result, tile = project(0)
    got[bat, seq, :pairs] = result
    got[bat, seq, pairs:] = tile
    flip_all(lead)

    @pl.when(bat == 1)
    def _():
        pl.semaphore_wait(barrier, 2 * (n_seq - 1))
        pl.semaphore_signal(all_sem, inc=1, device_id={"bat": peer}, device_id_type=MESH)

    @pl.when(bat == 0)
    def _():
        pl.semaphore_wait(all_sem, 1)

    early = n_seq // 4
    lax.fori_loop(0, early, send_own, 0)

    arrive(rest)
    score_all(rest, other)
    flip_all(rest)
    weigh_all((*lead, *rest))
    result, tile = project(1)
    sent[:pairs] = result
    sent[pairs:] = tile
    lax.fori_loop(0, early, send_peer, 0)

    def send_both(step, _):
        send_peer(step, 0)
        return send_own(step, 0)

    lax.fori_loop(early, n_seq, send_both, 0)

    def settle(ref, sem):
        pltpu.make_async_copy(ref, ref, sem).wait()

    few = pl.ds(0, n_seq - 1)
    settle(got.at[0, few], recv_sems.at[bat])
    settle(got.at[0], recv_sems.at[peer])

    lane = iota((group, depth), 1)
    sub = iota((group, depth), 0)
    picked = iota((pairs, depth), 0) == iota((pairs, depth), 1) % pairs
    for side in range(2):
        peaks, sizes = [], []
        for start in range(0, n_seq, group):
            peak = jnp.zeros((group, depth), jnp.float32)
            size = jnp.zeros((group, depth), jnp.float32)
            for j in range(group):
                tile = got[side, start + j, pairs:].astype(jnp.float32)
                top, sum_ = [
                    functools.reduce(jnp.add, [tile[k : k + 1] for k in range(at, at + pieces)])
                    for at in (0, pieces)
                ]
                peak = jnp.where(sub == j, top, peak)
                size = jnp.where(sub == j, sum_, size)
            peaks.append(peak)
            sizes.append(size)
        top = functools.reduce(jnp.maximum, peaks)
        top = jnp.max(top, axis=0, keepdims=True)
        factors = [jnp.exp(peak - top) for peak in peaks]
        whole = functools.reduce(jnp.add, [f * s for f, s in zip(factors, sizes)])
        inverse = 1.0 / jnp.sum(whole, axis=0, keepdims=True)
        spread = []
        for factor in factors:
            scaled = factor * inverse
            for start in range(0, group, copies):
                line = jnp.sum(
                    jnp.where(sub == start + lane // pairs, scaled, 0.0), axis=0, keepdims=True
                )
                spread.append(jnp.where(picked, line, 0.0))
        spread = jnp.concatenate(spread, axis=1)
        high = spread.astype(jnp.bfloat16)
        low = (spread - high.astype(jnp.float32)).astype(jnp.bfloat16)
        merged = jnp.dot(
            jnp.concatenate([high, low], axis=0),
            got[side, :, :pairs].reshape(n_seq * pairs, depth),
            preferred_element_type=jnp.float32,
        )
        merged = (merged[:pairs] + merged[pairs:]).reshape(half, heads, depth)
        out[:, side * heads : (side + 1) * heads, :] = merged.astype(jnp.bfloat16)

    settle(got.at[0], send_sems.at[1])
    settle(got.at[0, few], send_sems.at[0])


def per_device(n_seq, queries, latent_cache, cache_lengths, key_weight, value_weight):
    half, all_heads, _ = queries.shape
    heads = key_weight.shape[0]
    depth = value_weight.shape[2]
    pairs = half * heads
    latent = key_weight.shape[2]
    shard = latent_cache.shape[1]
    columns = jnp.swapaxes(latent_cache, 1, 2)
    vmem, anywhere = pltpu.VMEM, pl.BlockSpec(memory_space=pltpu.HBM)
    dma = pltpu.SemaphoreType.DMA
    operands = (cache_lengths, queries, columns, key_weight, value_weight)
    held = [pltpu.with_memory_space_constraint(x, pltpu.HBM) for x in operands]
    return pl.pallas_call(
        functools.partial(kernel, n_seq),
        out_shape=jax.ShapeDtypeStruct((half, all_heads, depth), jnp.bfloat16),
        in_specs=[anywhere] * 5,
        out_specs=pl.BlockSpec(memory_space=pltpu.VMEM),
        scratch_shapes=[
            pltpu.SMEM(cache_lengths.shape, cache_lengths.dtype),
            vmem(queries.shape, queries.dtype),
            vmem(queries.shape, queries.dtype),
            vmem(columns.shape, columns.dtype),
            vmem(key_weight.shape, key_weight.dtype),
            vmem(value_weight.shape, value_weight.dtype),
            vmem((2 * half, shard, latent), columns.dtype),
            vmem((2, n_seq, pairs + stat_rows, depth), jnp.bfloat16),
            vmem((pairs + stat_rows, depth), jnp.bfloat16),
            dma((4,)),
            dma((2 * half,)),
            dma((2,)),
            dma((2,)),
            dma((2,)),
            pltpu.SemaphoreType.REGULAR,
            pltpu.SemaphoreType.REGULAR,
        ],
        compiler_params=pltpu.CompilerParams(
            collective_id=0, has_side_effects=True, vmem_limit_bytes=32 << 20
        ),
    )(*held)


def solution(mesh):
    placed = (
        P(("grp", "bat"), None, None),
        P("grp", "seq", None),
        P("grp"),
        P("bat", None, None),
        P("bat", None, None),
    )
    return jax.shard_map(
        functools.partial(per_device, mesh.shape["seq"]),
        mesh=mesh,
        in_specs=placed,
        out_specs=P(("grp", "bat"), None, None),
        check_vma=False,
    )
```

```python
import functools

import jax
import jax.numpy as jnp
from jax import lax
from jax.experimental import pallas as pl
from jax.experimental.pallas import tpu as pltpu
from jax.sharding import PartitionSpec as P

MESH = pl.DeviceIdType.MESH
masked_score = -1e30
group = 8
pieces = 3
stat_rows = 2 * pieces


def iota(shape, dim):
    return lax.broadcasted_iota(jnp.int32, shape, dim)


def split3(x):
    parts = []
    for _ in range(pieces):
        part = x.astype(jnp.bfloat16).astype(jnp.float32)
        parts.append(part)
        x = x - part
    return parts


def kernel(
    n_seq,
    lengths_far,
    queries,
    cache,
    key_weight,
    value_weight,
    out,
    lengths,
    own_q,
    other_q,
    columns,
    keys,
    values,
    flipped,
    got,
    sent,
    load_sems,
    column_sems,
    query_sems,
    send_sems,
    recv_sems,
    near_sem,
    all_sem,
):
    seq = lax.axis_index("seq")
    bat = lax.axis_index("bat")
    peer = 1 - bat
    half, _, width = queries.shape
    heads, nope, latent = key_weight.shape
    depth = value_weight.shape[2]
    shard = cache.shape[2]
    pairs = half * heads
    copies = depth // pairs
    scaling = width ** (-0.5)

    load_q = pltpu.make_async_copy(queries, own_q, load_sems.at[0])
    load_k = pltpu.make_async_copy(key_weight, keys, load_sems.at[1])
    load_v = pltpu.make_async_copy(value_weight, values, load_sems.at[2])
    load_lengths = pltpu.make_async_copy(lengths_far, lengths, load_sems.at[3])
    load_columns = [
        pltpu.make_async_copy(
            cache.at[(bat if i < half else peer) * half + i % half], columns.at[i], column_sems.at[i]
        )
        for i in range(2 * half)
    ]

    def start_pieces(source, target, sem, parts):
        size = heads // parts
        for j in range(parts):
            piece = pl.ds(j * size, size)
            pltpu.make_async_copy(source.at[piece], target.at[piece], sem).start()

    load_q.start()
    start_pieces(key_weight, keys, load_sems.at[1], heads)
    for copy in load_columns[:half + 1]:
        copy.start()
    start_pieces(value_weight, values, load_sems.at[2], heads)
    for copy in load_columns[half + 1:]:
        copy.start()
    load_lengths.start()

    barrier = pltpu.get_barrier_semaphore()

    def greet(step, _):
        far = lax.rem(seq + step, n_seq)
        pl.semaphore_signal(
            barrier, inc=1, device_id={"seq": far, "bat": 1}, device_id_type=MESH
        )
        return 0

    @pl.when(bat == 1)
    def _():
        pl.semaphore_signal(barrier, inc=1, device_id={"bat": peer}, device_id_type=MESH)

    lax.fori_loop(1, n_seq, greet, 0)

    def joined_rows(q_ref):
        q = q_ref[...].astype(jnp.float32)
        mine = jnp.where(bat == 0, q[:, :heads], q[:, heads:]).reshape(pairs, width)
        plain = mine[:, :nope]
        head_of = iota((pairs, nope), 0) % heads
        spread = jnp.concatenate(
            [jnp.where(head_of == h, plain, 0.0) for h in range(heads)], axis=1
        ).astype(jnp.bfloat16)
        absorbed = jnp.dot(
            spread, keys[...].reshape(heads * nope, latent), preferred_element_type=jnp.float32
        )
        return jnp.concatenate([absorbed, mine[:, nope:]], axis=1)

    def score(joined, i):
        piece = joined[(i % half) * heads : (i % half + 1) * heads].astype(jnp.bfloat16)
        scores = lax.dot_general(
            piece, columns[i], (((1,), (0,)), ((), ())), preferred_element_type=jnp.float32
        )
        owner = bat if i < half else peer
        left = lengths[owner * half + i % half] - seq * shard
        return jnp.where(iota(scores.shape, 1) < left, scores * scaling, masked_score)

    def soften(scores):
        highest = jnp.max(scores, axis=1, keepdims=True)
        weights = jnp.exp(scores - highest)
        return highest, jnp.sum(weights, axis=1, keepdims=True), weights

    def flip(i):
        flipped[i] = columns[i, :latent].T

    def weigh(weights, i):
        blank = jnp.zeros((heads, shard), jnp.float32)
        rows = [weights if k == i % half else blank for k in range(half)]
        return jnp.dot(
            jnp.concatenate(rows, axis=0).astype(jnp.bfloat16),
            flipped[i],
            preferred_element_type=jnp.float32,
        )

    def send(source, far, side, index):
        return pltpu.make_async_remote_copy(
            src_ref=source,
            dst_ref=got.at[bat, seq],
            send_sem=send_sems.at[index],
            recv_sem=recv_sems.at[bat],
            device_id={"seq": far, "bat": side},
            device_id_type=MESH,
        )

    @pl.when(bat == 0)
    def _():
        pl.semaphore_wait(barrier, 1)
        pl.semaphore_signal(near_sem, inc=1, device_id={"bat": peer}, device_id_type=MESH)

    @pl.when(bat == 1)
    def _():
        pl.semaphore_wait(near_sem, 1)

    swap = pltpu.make_async_remote_copy(
        src_ref=own_q,
        dst_ref=other_q,
        send_sem=query_sems.at[0],
        recv_sem=query_sems.at[1],
        device_id={"bat": peer},
        device_id_type=MESH,
    )
    load_q.wait()
    swap.start()
    load_k.wait()
    joined = joined_rows(own_q)

    def project(side):
        stack = sums[side]
        head_of = iota((pairs, latent), 0) % heads
        spread = jnp.concatenate(
            [jnp.where(head_of == h, stack, 0.0).astype(jnp.bfloat16) for h in range(heads)], axis=1
        )
        result = jnp.dot(
            spread, values[...].reshape(heads * latent, depth), preferred_element_type=jnp.float32
        )
        sub = iota((stat_rows, depth), 0)
        rows = split3(jnp.sum(maxima[side], axis=0, keepdims=True))
        rows += split3(jnp.sum(totals[side], axis=0, keepdims=True))
        tile = jnp.zeros((stat_rows, depth), jnp.float32)
        for j, line in enumerate(rows):
            tile = jnp.where(sub == j, line, tile)
        return result.astype(jnp.bfloat16), tile.astype(jnp.bfloat16)

    def far_of(step):
        return jnp.where(2 * seq < n_seq, n_seq - 1 - step, step)

    def send_own(step, _):
        far = far_of(step)

        @pl.when(far != seq)
        def _():
            send(got.at[bat, seq], far, bat, 0).start()

        return 0

    def send_peer(step, _):
        send(sent, far_of(step), peer, 1).start()
        return 0

    lane = iota((heads, depth), 1)
    slot = lax.rem(lane, pairs)
    row = iota((heads, depth), 0)
    maxima = [jnp.zeros((heads, depth), jnp.float32)] * 2
    totals = [jnp.zeros((heads, depth), jnp.float32)] * 2
    sums, scores = [None, None], {}

    def arrive(items):
        for i in items:
            load_columns[i].wait()

    def score_all(items, joined):
        for i in items:
            scores[i] = score(joined, i)

    def flip_all(items):
        for i in items:
            flip(i)

    def weigh_all(items):
        weights = {}
        for i in items:
            side = i // half
            highest, total, weights[i] = soften(scores[i])
            here = slot == (i % half) * heads + row
            maxima[side] = jnp.where(here, highest, maxima[side])
            totals[side] = jnp.where(here, total, totals[side])
        for i in items:
            side = i // half
            part = weigh(weights[i], i)
            sums[side] = part if sums[side] is None else sums[side] + part

    first, second = range(half // 2), range(half // 2, half)
    lead, rest = (half,), range(half + 1, 2 * half)

    arrive(first)
    load_lengths.wait()
    score_all(first, joined)
    flip_all(first)

    swap.wait()
    arrive(second)
    score_all(second, joined)
    other = joined_rows(other_q)
    flip_all(second)
    weigh_all(first)

    load_v.wait()
    arrive(lead)
    weigh_all(second)
    score_all(lead, other)
    result, tile = project(0)
    got[bat, seq, :pairs] = result
    got[bat, seq, pairs:] = tile
    flip_all(lead)

    @pl.when(bat == 1)
    def _():
        pl.semaphore_wait(barrier, 2 * (n_seq - 1))
        pl.semaphore_signal(all_sem, inc=1, device_id={"bat": peer}, device_id_type=MESH)

    @pl.when(bat == 0)
    def _():
        pl.semaphore_wait(all_sem, 1)

    early = n_seq // 8
    lax.fori_loop(0, early, send_own, 0)

    arrive(rest)
    score_all(rest, other)
    flip_all(rest)
    weigh_all((*lead, *rest))
    result, tile = project(1)
    sent[:pairs] = result
    sent[pairs:] = tile
    lax.fori_loop(0, early, send_peer, 0)

    def send_both(step, _):
        send_own(step, 0)
        return send_peer(step, 0)

    lax.fori_loop(early, n_seq, send_both, 0)

    def settle(ref, sem):
        pltpu.make_async_copy(ref, ref, sem).wait()

    few = pl.ds(0, n_seq - 1)
    settle(got.at[0, few], recv_sems.at[bat])
    settle(got.at[0], recv_sems.at[peer])

    lane = iota((group, depth), 1)
    sub = iota((group, depth), 0)
    picked = iota((pairs, depth), 0) == iota((pairs, depth), 1) % pairs
    for side in range(2):
        peaks, sizes = [], []
        for start in range(0, n_seq, group):
            peak = jnp.zeros((group, depth), jnp.float32)
            size = jnp.zeros((group, depth), jnp.float32)
            for j in range(group):
                tile = got[side, start + j, pairs:].astype(jnp.float32)
                top, sum_ = [
                    functools.reduce(jnp.add, [tile[k : k + 1] for k in range(at, at + pieces)])
                    for at in (0, pieces)
                ]
                peak = jnp.where(sub == j, top, peak)
                size = jnp.where(sub == j, sum_, size)
            peaks.append(peak)
            sizes.append(size)
        top = functools.reduce(jnp.maximum, peaks)
        top = jnp.max(top, axis=0, keepdims=True)
        factors = [jnp.exp(peak - top) for peak in peaks]
        whole = functools.reduce(jnp.add, [f * s for f, s in zip(factors, sizes)])
        inverse = 1.0 / jnp.sum(whole, axis=0, keepdims=True)
        spread = []
        for factor in factors:
            scaled = factor * inverse
            for start in range(0, group, copies):
                line = jnp.sum(
                    jnp.where(sub == start + lane // pairs, scaled, 0.0), axis=0, keepdims=True
                )
                spread.append(jnp.where(picked, line, 0.0))
        spread = jnp.concatenate(spread, axis=1)
        high = spread.astype(jnp.bfloat16)
        low = (spread - high.astype(jnp.float32)).astype(jnp.bfloat16)
        merged = jnp.dot(
            jnp.concatenate([high, low], axis=0),
            got[side, :, :pairs].reshape(n_seq * pairs, depth),
            preferred_element_type=jnp.float32,
        )
        merged = (merged[:pairs] + merged[pairs:]).reshape(half, heads, depth)
        out[:, side * heads : (side + 1) * heads, :] = merged.astype(jnp.bfloat16)

    settle(got.at[0], send_sems.at[1])
    settle(got.at[0, few], send_sems.at[0])


def per_device(n_seq, queries, latent_cache, cache_lengths, key_weight, value_weight):
    half, all_heads, _ = queries.shape
    heads = key_weight.shape[0]
    depth = value_weight.shape[2]
    pairs = half * heads
    latent = key_weight.shape[2]
    shard = latent_cache.shape[1]
    columns = jnp.swapaxes(latent_cache, 1, 2)
    vmem, anywhere = pltpu.VMEM, pl.BlockSpec(memory_space=pltpu.HBM)
    dma = pltpu.SemaphoreType.DMA
    operands = (cache_lengths, queries, columns, key_weight, value_weight)
    held = [pltpu.with_memory_space_constraint(x, pltpu.HBM) for x in operands]
    return pl.pallas_call(
        functools.partial(kernel, n_seq),
        out_shape=jax.ShapeDtypeStruct((half, all_heads, depth), jnp.bfloat16),
        in_specs=[anywhere] * 5,
        out_specs=pl.BlockSpec(memory_space=pltpu.VMEM),
        scratch_shapes=[
            pltpu.SMEM(cache_lengths.shape, cache_lengths.dtype),
            vmem(queries.shape, queries.dtype),
            vmem(queries.shape, queries.dtype),
            vmem(columns.shape, columns.dtype),
            vmem(key_weight.shape, key_weight.dtype),
            vmem(value_weight.shape, value_weight.dtype),
            vmem((2 * half, shard, latent), columns.dtype),
            vmem((2, n_seq, pairs + stat_rows, depth), jnp.bfloat16),
            vmem((pairs + stat_rows, depth), jnp.bfloat16),
            dma((4,)),
            dma((2 * half,)),
            dma((2,)),
            dma((2,)),
            dma((2,)),
            pltpu.SemaphoreType.REGULAR,
            pltpu.SemaphoreType.REGULAR,
        ],
        compiler_params=pltpu.CompilerParams(
            collective_id=0, has_side_effects=True, vmem_limit_bytes=32 << 20
        ),
    )(*held)


def solution(mesh):
    placed = (
        P(("grp", "bat"), None, None),
        P("grp", "seq", None),
        P("grp"),
        P("bat", None, None),
        P("bat", None, None),
    )
    return jax.shard_map(
        functools.partial(per_device, mesh.shape["seq"]),
        mesh=mesh,
        in_specs=placed,
        out_specs=P(("grp", "bat"), None, None),
        check_vma=False,
    )
```

```python
import functools

import jax
import jax.numpy as jnp
from jax import lax
from jax.experimental import pallas as pl
from jax.experimental.pallas import tpu as pltpu
from jax.sharding import PartitionSpec as P

MESH = pl.DeviceIdType.MESH
masked_score = -1e30
group = 8
pieces = 3
stat_rows = 2 * pieces


def iota(shape, dim):
    return lax.broadcasted_iota(jnp.int32, shape, dim)


def split3(x):
    parts = []
    for _ in range(pieces):
        part = x.astype(jnp.bfloat16).astype(jnp.float32)
        parts.append(part)
        x = x - part
    return parts


def kernel(
    n_seq,
    lengths_far,
    queries,
    cache,
    key_weight,
    value_weight,
    out,
    lengths,
    own_q,
    other_q,
    columns,
    keys,
    values,
    flipped,
    got,
    sent,
    load_sems,
    column_sems,
    query_sems,
    send_sems,
    recv_sems,
    near_sem,
    all_sem,
):
    seq = lax.axis_index("seq")
    bat = lax.axis_index("bat")
    peer = 1 - bat
    half, _, width = queries.shape
    heads, nope, latent = key_weight.shape
    depth = value_weight.shape[2]
    shard = cache.shape[2]
    pairs = half * heads
    copies = depth // pairs
    scaling = width ** (-0.5)

    load_q = pltpu.make_async_copy(queries, own_q, load_sems.at[0])
    load_k = pltpu.make_async_copy(key_weight, keys, load_sems.at[1])
    load_v = pltpu.make_async_copy(value_weight, values, load_sems.at[2])
    load_lengths = pltpu.make_async_copy(lengths_far, lengths, load_sems.at[3])
    load_columns = [
        pltpu.make_async_copy(
            cache.at[(bat if i < half else peer) * half + i % half], columns.at[i], column_sems.at[i]
        )
        for i in range(2 * half)
    ]

    def start_pieces(source, target, sem, parts):
        size = heads // parts
        for j in range(parts):
            piece = pl.ds(j * size, size)
            pltpu.make_async_copy(source.at[piece], target.at[piece], sem).start()

    load_q.start()
    start_pieces(key_weight, keys, load_sems.at[1], heads)
    for copy in load_columns[:half + 1]:
        copy.start()
    start_pieces(value_weight, values, load_sems.at[2], heads)
    for copy in load_columns[half + 1:]:
        copy.start()
    load_lengths.start()

    barrier = pltpu.get_barrier_semaphore()

    def greet(step, _):
        far = lax.rem(seq + step, n_seq)
        pl.semaphore_signal(
            barrier, inc=1, device_id={"seq": far, "bat": 1}, device_id_type=MESH
        )
        return 0

    @pl.when(bat == 1)
    def _():
        pl.semaphore_signal(barrier, inc=1, device_id={"bat": peer}, device_id_type=MESH)

    def joined_rows(q_ref):
        q = q_ref[...].astype(jnp.float32)
        mine = jnp.where(bat == 0, q[:, :heads], q[:, heads:]).reshape(pairs, width)
        plain = mine[:, :nope]
        head_of = iota((pairs, nope), 0) % heads
        spread = jnp.concatenate(
            [jnp.where(head_of == h, plain, 0.0) for h in range(heads)], axis=1
        ).astype(jnp.bfloat16)
        absorbed = jnp.dot(
            spread, keys[...].reshape(heads * nope, latent), preferred_element_type=jnp.float32
        )
        return jnp.concatenate([absorbed, mine[:, nope:]], axis=1)

    def score(joined, i):
        piece = joined[(i % half) * heads : (i % half + 1) * heads].astype(jnp.bfloat16)
        scores = lax.dot_general(
            piece, columns[i], (((1,), (0,)), ((), ())), preferred_element_type=jnp.float32
        )
        owner = bat if i < half else peer
        left = lengths[owner * half + i % half] - seq * shard
        return jnp.where(iota(scores.shape, 1) < left, scores * scaling, masked_score)

    def soften(scores):
        highest = jnp.max(scores, axis=1, keepdims=True)
        weights = jnp.exp(scores - highest)
        return highest, jnp.sum(weights, axis=1, keepdims=True), weights

    def flip(i):
        flipped[i] = columns[i, :latent].T

    def weigh(weights, i):
        blank = jnp.zeros((heads, shard), jnp.float32)
        rows = [weights if k == i % half else blank for k in range(half)]
        return jnp.dot(
            jnp.concatenate(rows, axis=0).astype(jnp.bfloat16),
            flipped[i],
            preferred_element_type=jnp.float32,
        )

    def send(source, far, side, index):
        return pltpu.make_async_remote_copy(
            src_ref=source,
            dst_ref=got.at[bat, seq],
            send_sem=send_sems.at[index],
            recv_sem=recv_sems.at[bat],
            device_id={"seq": far, "bat": side},
            device_id_type=MESH,
        )

    @pl.when(bat == 0)
    def _():
        pl.semaphore_wait(barrier, 1)
        pl.semaphore_signal(near_sem, inc=1, device_id={"bat": peer}, device_id_type=MESH)

    @pl.when(bat == 1)
    def _():
        pl.semaphore_wait(near_sem, 1)

    swap = pltpu.make_async_remote_copy(
        src_ref=own_q,
        dst_ref=other_q,
        send_sem=query_sems.at[0],
        recv_sem=query_sems.at[1],
        device_id={"bat": peer},
        device_id_type=MESH,
    )
    lax.fori_loop(1, n_seq, greet, 0)
    load_q.wait()
    swap.start()
    load_k.wait()
    joined = joined_rows(own_q)

    def project(side):
        stack = sums[side]
        head_of = iota((pairs, latent), 0) % heads
        spread = jnp.concatenate(
            [jnp.where(head_of == h, stack, 0.0).astype(jnp.bfloat16) for h in range(heads)], axis=1
        )
        result = jnp.dot(
            spread, values[...].reshape(heads * latent, depth), preferred_element_type=jnp.float32
        )
        sub = iota((stat_rows, depth), 0)
        rows = split3(jnp.sum(maxima[side], axis=0, keepdims=True))
        rows += split3(jnp.sum(totals[side], axis=0, keepdims=True))
        tile = jnp.zeros((stat_rows, depth), jnp.float32)
        for j, line in enumerate(rows):
            tile = jnp.where(sub == j, line, tile)
        return result.astype(jnp.bfloat16), tile.astype(jnp.bfloat16)

    def far_of(step):
        return jnp.where(2 * seq < n_seq, n_seq - 1 - step, step)

    def send_own(step, _):
        far = far_of(step)

        @pl.when(far != seq)
        def _():
            send(got.at[bat, seq], far, bat, 0).start()

        return 0

    def send_peer(step, _):
        send(sent, far_of(step), peer, 1).start()
        return 0

    lane = iota((heads, depth), 1)
    slot = lax.rem(lane, pairs)
    row = iota((heads, depth), 0)
    maxima = [jnp.zeros((heads, depth), jnp.float32)] * 2
    totals = [jnp.zeros((heads, depth), jnp.float32)] * 2
    sums, scores = [None, None], {}

    def arrive(items):
        for i in items:
            load_columns[i].wait()

    def score_all(items, joined):
        for i in items:
            scores[i] = score(joined, i)

    def flip_all(items):
        for i in items:
            flip(i)

    def weigh_all(items):
        weights = {}
        for i in items:
            side = i // half
            highest, total, weights[i] = soften(scores[i])
            here = slot == (i % half) * heads + row
            maxima[side] = jnp.where(here, highest, maxima[side])
            totals[side] = jnp.where(here, total, totals[side])
        for i in items:
            side = i // half
            part = weigh(weights[i], i)
            sums[side] = part if sums[side] is None else sums[side] + part

    first, second = range(half // 2), range(half // 2, half)
    lead, rest = (half,), range(half + 1, 2 * half)

    arrive(first)
    load_lengths.wait()
    score_all(first, joined)
    flip_all(first)

    swap.wait()
    arrive(second)
    score_all(second, joined)
    other = joined_rows(other_q)
    flip_all(second)
    weigh_all(first)

    load_v.wait()
    arrive(lead)
    weigh_all(second)
    score_all(lead, other)
    result, tile = project(0)
    got[bat, seq, :pairs] = result
    got[bat, seq, pairs:] = tile
    flip_all(lead)

    @pl.when(bat == 1)
    def _():
        pl.semaphore_wait(barrier, 2 * (n_seq - 1))
        pl.semaphore_signal(all_sem, inc=1, device_id={"bat": peer}, device_id_type=MESH)

    @pl.when(bat == 0)
    def _():
        pl.semaphore_wait(all_sem, 1)

    early = n_seq // 8
    lax.fori_loop(0, early, send_own, 0)

    arrive(rest)
    score_all(rest, other)
    flip_all(rest)
    weigh_all((*lead, *rest))
    result, tile = project(1)
    sent[:pairs] = result
    sent[pairs:] = tile
    lax.fori_loop(0, early, send_peer, 0)

    def send_both(step, _):
        send_own(step, 0)
        return send_peer(step, 0)

    lax.fori_loop(early, n_seq, send_both, 0)

    def settle(ref, sem):
        pltpu.make_async_copy(ref, ref, sem).wait()

    few = pl.ds(0, n_seq - 1)
    settle(got.at[0, few], recv_sems.at[bat])
    settle(got.at[0], recv_sems.at[peer])

    lane = iota((group, depth), 1)
    sub = iota((group, depth), 0)
    picked = iota((pairs, depth), 0) == iota((pairs, depth), 1) % pairs
    for side in range(2):
        peaks, sizes = [], []
        for start in range(0, n_seq, group):
            peak = jnp.zeros((group, depth), jnp.float32)
            size = jnp.zeros((group, depth), jnp.float32)
            for j in range(group):
                tile = got[side, start + j, pairs:].astype(jnp.float32)
                top, sum_ = [
                    functools.reduce(jnp.add, [tile[k : k + 1] for k in range(at, at + pieces)])
                    for at in (0, pieces)
                ]
                peak = jnp.where(sub == j, top, peak)
                size = jnp.where(sub == j, sum_, size)
            peaks.append(peak)
            sizes.append(size)
        top = functools.reduce(jnp.maximum, peaks)
        top = jnp.max(top, axis=0, keepdims=True)
        factors = [jnp.exp(peak - top) for peak in peaks]
        whole = functools.reduce(jnp.add, [f * s for f, s in zip(factors, sizes)])
        inverse = 1.0 / jnp.sum(whole, axis=0, keepdims=True)
        spread = []
        for factor in factors:
            scaled = factor * inverse
            for start in range(0, group, copies):
                line = jnp.sum(
                    jnp.where(sub == start + lane // pairs, scaled, 0.0), axis=0, keepdims=True
                )
                spread.append(jnp.where(picked, line, 0.0))
        spread = jnp.concatenate(spread, axis=1)
        high = spread.astype(jnp.bfloat16)
        low = (spread - high.astype(jnp.float32)).astype(jnp.bfloat16)
        merged = jnp.dot(
            jnp.concatenate([high, low], axis=0),
            got[side, :, :pairs].reshape(n_seq * pairs, depth),
            preferred_element_type=jnp.float32,
        )
        merged = (merged[:pairs] + merged[pairs:]).reshape(half, heads, depth)
        out[:, side * heads : (side + 1) * heads, :] = merged.astype(jnp.bfloat16)

    settle(got.at[0], send_sems.at[1])
    settle(got.at[0, few], send_sems.at[0])


def per_device(n_seq, queries, latent_cache, cache_lengths, key_weight, value_weight):
    half, all_heads, _ = queries.shape
    heads = key_weight.shape[0]
    depth = value_weight.shape[2]
    pairs = half * heads
    latent = key_weight.shape[2]
    shard = latent_cache.shape[1]
    columns = jnp.swapaxes(latent_cache, 1, 2)
    vmem, anywhere = pltpu.VMEM, pl.BlockSpec(memory_space=pltpu.HBM)
    dma = pltpu.SemaphoreType.DMA
    operands = (cache_lengths, queries, columns, key_weight, value_weight)
    held = [pltpu.with_memory_space_constraint(x, pltpu.HBM) for x in operands]
    return pl.pallas_call(
        functools.partial(kernel, n_seq),
        out_shape=jax.ShapeDtypeStruct((half, all_heads, depth), jnp.bfloat16),
        in_specs=[anywhere] * 5,
        out_specs=pl.BlockSpec(memory_space=pltpu.VMEM),
        scratch_shapes=[
            pltpu.SMEM(cache_lengths.shape, cache_lengths.dtype),
            vmem(queries.shape, queries.dtype),
            vmem(queries.shape, queries.dtype),
            vmem(columns.shape, columns.dtype),
            vmem(key_weight.shape, key_weight.dtype),
            vmem(value_weight.shape, value_weight.dtype),
            vmem((2 * half, shard, latent), columns.dtype),
            vmem((2, n_seq, pairs + stat_rows, depth), jnp.bfloat16),
            vmem((pairs + stat_rows, depth), jnp.bfloat16),
            dma((4,)),
            dma((2 * half,)),
            dma((2,)),
            dma((2,)),
            dma((2,)),
            pltpu.SemaphoreType.REGULAR,
            pltpu.SemaphoreType.REGULAR,
        ],
        compiler_params=pltpu.CompilerParams(
            collective_id=0, has_side_effects=True, vmem_limit_bytes=32 << 20
        ),
    )(*held)


def solution(mesh):
    placed = (
        P(("grp", "bat"), None, None),
        P("grp", "seq", None),
        P("grp"),
        P("bat", None, None),
        P("bat", None, None),
    )
    return jax.shard_map(
        functools.partial(per_device, mesh.shape["seq"]),
        mesh=mesh,
        in_specs=placed,
        out_specs=P(("grp", "bat"), None, None),
        check_vma=False,
    )
```
